32 devices in a mesh: section: 4 (over x, core), mp: 8 (over z, y).
Axes of the slice: x: 2, y: 2, z: 4, core: 2. Of those that a mesh axis runs over, the one named last changes fastest.
Arguments:
- encoder_input: bfloat16 [576, 1024], P('section'), may hold values from -6 to 6
- input_gain: float32 [1024], replicated, may hold values from 0.1 to 1.9
- expand_weight: bfloat16 [1024, 8192], P(None, 'mp'), may hold values from -0.1875 to 0.1875
- reduce_weight: bfloat16 [8192, 1024], P('mp'), may hold values from -0.0625 to 0.0625
- final_gain: float32 [1024], replicated, may hold values from 0.1 to 1.9
- decoder_input: bfloat16 [1024, 1024], P('section'), may hold values from -6 to 6
- query_gain: float32 [1024], replicated, may hold values from 0.1 to 1.9
- query_weight: bfloat16 [1024, 2048], P(None, 'mp'), may hold values from -2 to 2
- key_weight: bfloat16 [1024, 2048], P(None, 'mp'), may hold values from -0.1875 to 0.1875
- value_weight: bfloat16 [1024, 2048], P(None, 'mp'), may hold values from -0.1875 to 0.1875
- mixing_weight: bfloat16 [2048, 1024], P('mp'), may hold values from -0.125 to 0.125
- output_gradient: bfloat16 [1024, 1024], P('section'), may hold values from -84 to 84
Outputs:
- memory: bfloat16 [576, 1024], P(('section', 'mp'))
- memory_gradient: bfloat16 [576, 1024], P(('section', 'mp'))
The draws below stay inside these ranges and needn't reach their ends.
All inputs are finite; a program needn't handle non-finite values.
Results may differ from the reference program's by a relative error of at most 0.025.
The reference program's roundings to bfloat16 on the way (of `normed`, `hidden`, `dec_normed`, `queries` and `head_grad`) count: a program that leaves them out, or rounds other values in their place, can miss the bound.
Values may be sent and summed in bfloat16 or wider, within the bound.
No kernel may reach another device: no remote copies, remote signals or barrier semaphores. Data moves between devices by JAX's collectives and lax.ppermute only.
A program may use at most 64 MiB of HBM per device.

```python
import jax
import jax.numpy as jnp
from jax import lax

D = 1024
DK = 128
FF = 8192
HEADS = 16
INNER = 2048
ENC_TOTAL = 576
DEC_TOTAL = 1024


def draw_query_weight(key, part):
    second = jax.random.fold_in(jax.random.fold_in(key, 11), 1)
    values = jax.random.normal(second, (D, INNER), jnp.float32) / D ** 0.5
    values = jnp.clip(values, -6.0 / D ** 0.5, 6.0 / D ** 0.5)
    return jnp.clip(values, -2.0, 2.0).astype(jnp.bfloat16)


def levels(key, dims, cuts, low, high):
    def one(position, shards_of):
        draws = jax.random.uniform(jax.random.fold_in(jax.random.fold_in(key, 6), position), (shards_of,), jnp.float32, low / len(cuts), high / len(cuts))
        return jnp.repeat(jnp.exp(draws), dims[position] // shards_of).reshape((-1,) + (1,) * (len(dims) - position - 1))

    level = one(*cuts[0])
    for cut in cuts[1:]:
        level = level * one(*cut)
    return level


def scatter_about(own_key, dims, scale, reach, cuts=(), kind=jnp.bfloat16):
    values = scale * jax.random.normal(own_key, dims, jnp.float32)
    if cuts:
        values = values * levels(own_key, dims, cuts, -0.22, 0.18)
    return jnp.clip(values, -reach, reach).astype(kind)


def setup_inputs(seed: int = 0) -> dict:
    splits = jax.random.split(jax.random.key(seed), 13)
    encoder_input = scatter_about(splits[0], (ENC_TOTAL, D), 1.0, 6.0, ((0, 4),))
    input_gain = jnp.clip(1.0 + 0.18 * jax.random.normal(splits[1], (D,), jnp.float32), 0.1, 1.9)
    expand_weight = scatter_about(splits[2], (D, FF), D ** -0.5, 0.1875, ((1, 8),))
    reduce_weight = scatter_about(splits[3], (FF, D), FF ** -0.5, 0.0625, ((0, 8),))
    final_gain = jnp.clip(1.0 + 0.18 * jax.random.normal(splits[4], (D,), jnp.float32), 0.1, 1.9)
    decoder_input = scatter_about(splits[5], (DEC_TOTAL, D), 1.0, 6.0, ((0, 4),))
    query_gain = jnp.clip(1.0 + 0.18 * jax.random.normal(splits[6], (D,), jnp.float32), 0.1, 1.9)
    query_weight = draw_query_weight(jax.random.fold_in(splits[12], 71), 0)
    key_weight = scatter_about(splits[8], (D, INNER), D ** -0.5, 0.1875, ((1, 8),))
    value_weight = scatter_about(splits[9], (D, INNER), D ** -0.5, 0.1875, ((1, 8),))
    mixing_weight = scatter_about(splits[10], (INNER, D), INNER ** -0.5, 0.125, ((0, 8),))
    output_gradient = scatter_about(splits[11], (DEC_TOTAL, D), (ENC_TOTAL // 40), 84.0, ((0, 4),))
    return dict(encoder_input=encoder_input, input_gain=input_gain, expand_weight=expand_weight, reduce_weight=reduce_weight, final_gain=final_gain, decoder_input=decoder_input, query_gain=query_gain, query_weight=query_weight, key_weight=key_weight, value_weight=value_weight, mixing_weight=mixing_weight, output_gradient=output_gradient)


def norm_rows(rows, gain):
    values = rows.astype(jnp.float32)
    return values * lax.rsqrt(lax.optimization_barrier(jnp.mean(values * values, axis=-1, keepdims=True)) + 1e-06) * gain

def one_head(operands):
    query_block, key_block, value_block, grad_block = operands
    scale = DK ** (-0.5)
    scores = jnp.dot(query_block, key_block.T, preferred_element_type=jnp.float32) * scale
    probs = jax.nn.softmax(scores, axis=-1)
    prob_grad = jnp.dot(grad_block, value_block.T, preferred_element_type=jnp.float32)
    delta = lax.optimization_barrier(jnp.sum(probs * prob_grad, axis=-1, keepdims=True))
    score_grad = (probs * (prob_grad - delta) * scale).astype(jnp.bfloat16)
    probs_low = probs.astype(jnp.bfloat16)
    key_grad = jnp.dot(score_grad.T, query_block, preferred_element_type=jnp.float32).astype(jnp.bfloat16)
    value_grad = jnp.dot(probs_low.T, grad_block, preferred_element_type=jnp.float32).astype(jnp.bfloat16)
    return (key_grad, value_grad)

def split_heads(matrix):
    return matrix.reshape(matrix.shape[0], HEADS, DK).transpose(1, 0, 2)

def reference(encoder_input, input_gain, expand_weight, reduce_weight, final_gain, decoder_input, query_gain, query_weight, key_weight, value_weight, mixing_weight, output_gradient):
    normed = norm_rows(encoder_input, input_gain).astype(jnp.bfloat16)
    hidden = jnp.maximum(jnp.dot(normed, expand_weight, preferred_element_type=jnp.float32), 0.0).astype(jnp.bfloat16)
    residual_sum = encoder_input.astype(jnp.float32) + jnp.dot(hidden, reduce_weight, preferred_element_type=jnp.float32)
    memory = norm_rows(residual_sum, final_gain).astype(jnp.bfloat16)
    dec_normed = norm_rows(decoder_input, query_gain).astype(jnp.bfloat16)
    queries = jnp.dot(dec_normed, query_weight, preferred_element_type=jnp.float32).astype(jnp.bfloat16)
    keys = jnp.dot(memory, key_weight, preferred_element_type=jnp.float32).astype(jnp.bfloat16)
    values = jnp.dot(memory, value_weight, preferred_element_type=jnp.float32).astype(jnp.bfloat16)
    head_grad = jnp.dot(output_gradient, mixing_weight.T, preferred_element_type=jnp.float32).astype(jnp.bfloat16)
    key_heads, value_heads = lax.map(one_head, (split_heads(queries), split_heads(keys), split_heads(values), split_heads(head_grad)))
    key_grad = key_heads.transpose(1, 0, 2).reshape(keys.shape[0], HEADS * DK)
    value_grad = value_heads.transpose(1, 0, 2).reshape(keys.shape[0], HEADS * DK)
    memory_gradient = jnp.dot(key_grad, key_weight.T, preferred_element_type=jnp.float32) + jnp.dot(value_grad, value_weight.T, preferred_element_type=jnp.float32)
    return (memory, memory_gradient.astype(jnp.bfloat16))
```

```python
import jax
import jax.numpy as jnp
from jax import lax
from jax.sharding import PartitionSpec as P

DK = 128
LANES = 128


def norm_rows(rows, gain):
    values = rows.astype(jnp.float32)
    return values * lax.rsqrt(jnp.mean(values * values, axis=-1, keepdims=True) + 1e-06) * gain


def spread_sum(partial_value, own, axis):
    n = lax.axis_size(axis)
    rows, width = partial_value.shape
    if width % (n * LANES):
        return (own.astype(jnp.float32) + lax.psum(partial_value, axis)).astype(jnp.bfloat16)
    share = width // n
    blocks = jnp.stack(
        [partial_value[:, k * share : (k + 1) * share].astype(jnp.bfloat16) for k in range(n)]
    )
    arrived = lax.all_to_all(blocks, axis, 0, 0)
    mine = lax.dynamic_slice_in_dim(own, lax.axis_index(axis) * share, share, 1)
    total = mine.astype(jnp.float32) + jnp.sum(arrived.astype(jnp.float32), axis=0)
    total = total.astype(jnp.bfloat16)
    everything = lax.all_to_all(jnp.broadcast_to(total[None], (n,) + total.shape), axis, 0, 0)
    return jnp.concatenate([everything[k] for k in range(n)], axis=1)


def scatter_sum(partial_value, axis):
    n = lax.axis_size(axis)
    rows, width = partial_value.shape
    blocks = partial_value.reshape(n, rows // n, width // LANES, LANES).astype(jnp.bfloat16)
    arrived = lax.all_to_all(blocks, axis, 0, 0)
    return jnp.sum(arrived.astype(jnp.float32), axis=0).astype(jnp.bfloat16).reshape(rows // n, width)


def body(
    encoder_input,
    input_gain,
    expand_weight,
    reduce_weight,
    final_gain,
    decoder_input,
    query_gain,
    query_weight,
    key_weight,
    value_weight,
    mixing_weight,
    output_gradient,
):
    scale = DK ** (-0.5)
    heads = key_weight.shape[1] // DK
    width = heads * DK
    sections = lax.axis_size("section")
    dec_normed = norm_rows(decoder_input, query_gain).astype(jnp.bfloat16)
    queries = jnp.dot(dec_normed, query_weight, preferred_element_type=jnp.float32).astype(
        jnp.bfloat16
    )
    head_grad = jnp.einsum(
        "qd,id->qi", output_gradient, mixing_weight, preferred_element_type=jnp.float32
    ).astype(jnp.bfloat16)
    both = jnp.concatenate([queries, head_grad], axis=1)
    pieces = [both] + [
        lax.ppermute(both, "section", [(j, j ^ k) for j in range(sections)])
        for k in range(1, sections)
    ]

    normed = norm_rows(encoder_input, input_gain).astype(jnp.bfloat16)
    hidden = jnp.maximum(
        jnp.dot(normed, expand_weight, preferred_element_type=jnp.float32), 0.0
    ).astype(jnp.bfloat16)
    partial_value = jnp.dot(hidden, reduce_weight, preferred_element_type=jnp.float32)
    residual = spread_sum(partial_value, encoder_input, "mp")
    memory = norm_rows(residual, final_gain).astype(jnp.bfloat16)
    share = encoder_input.shape[0] // lax.axis_size("mp")
    memory_own = lax.dynamic_slice_in_dim(memory, lax.axis_index("mp") * share, share, 0)
    keys = jnp.dot(memory, key_weight, preferred_element_type=jnp.float32).astype(jnp.bfloat16)
    values = jnp.dot(memory, value_weight, preferred_element_type=jnp.float32).astype(jnp.bfloat16)

    everything = jnp.concatenate(pieces, axis=0)
    tokens = everything.shape[0]
    query_heads = everything[:, :width].reshape(tokens, heads, DK)
    grad_heads = everything[:, width:].reshape(tokens, heads, DK)
    key_heads = keys.reshape(keys.shape[0], heads, DK)
    value_heads = values.reshape(values.shape[0], heads, DK)
    scores = (
        jnp.einsum("qhd,khd->hqk", query_heads, key_heads, preferred_element_type=jnp.float32)
        * scale
    )
    local_top = jnp.max(scores, axis=-1)
    weights = jnp.exp(scores - local_top[..., None])
    prob_grad = jnp.einsum(
        "qhd,khd->hqk", grad_heads, value_heads, preferred_element_type=jnp.float32
    )
    stats = jnp.stack(
        [local_top, jnp.sum(weights, axis=-1), jnp.sum(weights * prob_grad, axis=-1)]
    )
    blocks = stats.reshape(3, heads, sections, tokens // sections)
    me = lax.axis_index("section")
    order = lax.bitwise_xor(jnp.arange(sections), me)
    ordered = jnp.take(blocks, order, axis=2)
    all_stats = lax.all_gather(ordered, "section", axis=0)
    tops, totals, numers = all_stats[:, 0], all_stats[:, 1], all_stats[:, 2]
    top = jnp.max(tops, axis=0)
    factor = jnp.exp(tops - top)
    total = jnp.sum(totals * factor, axis=0)
    numer = jnp.sum(numers * factor, axis=0)
    merged = jnp.take(jnp.stack([top, total, numer]), order, axis=2).reshape(3, heads, tokens)
    top, total, numer = merged[0], merged[1], merged[2]
    probs = weights * (jnp.exp(local_top - top) / total)[..., None]
    delta = (numer / total)[..., None]
    score_grad = (probs * (prob_grad - delta) * scale).astype(jnp.bfloat16)
    key_grad = (
        jnp.einsum("hqk,qhd->khd", score_grad, query_heads, preferred_element_type=jnp.float32)
        .reshape(keys.shape[0], width)
        .astype(jnp.bfloat16)
    )
    value_grad = (
        jnp.einsum(
            "hqk,qhd->khd",
            probs.astype(jnp.bfloat16),
            grad_heads,
            preferred_element_type=jnp.float32,
        )
        .reshape(keys.shape[0], width)
        .astype(jnp.bfloat16)
    )
    first = jnp.einsum("ki,di->kd", key_grad, key_weight, preferred_element_type=jnp.float32)
    second = jnp.einsum("ki,di->kd", value_grad, value_weight, preferred_element_type=jnp.float32)
    return (memory_own, scatter_sum(first + second, "mp"))


def solution(mesh):
    in_specs = (
        P("section", None),
        P(),
        P(None, "mp"),
        P("mp", None),
        P(),
        P("section", None),
        P(),
        P(None, "mp"),
        P(None, "mp"),
        P(None, "mp"),
        P("mp", None),
        P("section", None),
    )
    out_specs = (P(("section", "mp"), None), P(("section", "mp"), None))
    return jax.shard_map(body, mesh=mesh, in_specs=in_specs, out_specs=out_specs, check_vma=False)
```
